32 devices in a mesh: dp: 8 (over z, x), mp: 4 (over y, core).
Axes of the slice: x: 2, y: 2, z: 4, core: 2. Of those that a mesh axis runs over, the one named last changes fastest.
Arguments:
- grad_blocks: bfloat16 [16, 128, 128], P('dp', None, 'mp'), may hold values from -0.5 to 0.5
- owner_table: int32 [16], replicated, may hold values from 0 to 7, as said below
- prev_stats: float32 [64, 2, 128, 128], P('dp'), as said below
Outputs:
- update: bfloat16 [16, 128, 128], P('dp', None, 'mp')
- new_stats: float32 [64, 2, 128, 128], P('dp')
- inv_roots: float32 [64, 2, 128, 128], P('dp')
The draws below stay inside these ranges and needn't reach their ends.
Inputs may be any that keep to these rules, and one draw needn't show every extreme that they name: `owner_table`: every entry is a dp index; no index appears more than 8 times, and some index appears exactly 8 times. `prev_stats`: each [128, 128] matrix is symmetric positive semidefinite.
All inputs are finite; a program needn't handle non-finite values.
Results may differ from the reference program's by a relative error of at most 0.001.
Values may be sent and summed in bfloat16 or wider, within the bound.
A program may use at most 64 MiB of HBM per device.

```python
import jax
import jax.numpy as jnp
from jax import lax

BLOCK = 128
BLK_DEV = 2
ITERS = 16
NBLK = 16
CAP = 8
N_DP = 8


def draw_owner_table(key, part):
    dev_count = NBLK // BLK_DEV
    slot_count = dev_count * CAP
    base = jax.random.fold_in(key, 17)
    key_bias, key_noise, key_pick, key_order = jax.random.split(base, 4)
    weights = jax.random.randint(key_bias, (dev_count,), 0, 2).astype(jnp.int32)
    noise = jax.random.randint(key_noise, (slot_count,), 0, 2048).astype(jnp.int32)
    favored = jax.random.randint(key_pick, (), 0, dev_count).astype(jnp.int32)
    slot_range = jnp.arange(slot_count, dtype=jnp.int32)
    slot_owner = slot_range // CAP
    forced = (slot_range == 0) | (slot_range == (dev_count - 1) * CAP)
    score = weights[slot_owner] * 1024 + noise + jnp.where(slot_owner == favored, 8192, 0).astype(jnp.int32)
    score = score + jnp.where(forced, 16384, 0).astype(jnp.int32)
    score = score * slot_count + slot_range
    unused_vals, chosen = lax.top_k(score, NBLK)
    shuffled = jax.random.permutation(key_order, chosen)
    return (shuffled // CAP).astype(jnp.int32)


def draw_prev_stats(key, part):
    dev_count = NBLK // BLK_DEV
    count = dev_count * CAP * 2
    base = jax.random.fold_in(key, 29)
    key_mat, key_scale = jax.random.split(base, 2)
    factors = jax.random.normal(key_mat, (count, BLOCK, BLOCK), jnp.float32)
    product = jnp.einsum('pik,pjk->pij', factors, factors) / BLOCK
    product = 0.5 * (product + jnp.swapaxes(product, 1, 2))
    return product.reshape(dev_count * CAP, 2, BLOCK, BLOCK).astype(jnp.float32)


def shard_levels(stream_key, extent, cuts, low, largest):
    gain, own = 1.0, jax.random.fold_in(stream_key, 6)
    for dim, blocks in cuts:
        steps = jnp.exp(jax.random.uniform(jax.random.fold_in(own, dim), (blocks,), jnp.float32, low / len(cuts), largest / len(cuts)))
        gain = gain * jnp.repeat(steps, extent[dim] // blocks).reshape([-1 if axis == dim else 1 for axis in range(len(extent))])
    return gain


def centred(stream_key, dims, scale, limit, shards=(), kind=jnp.bfloat16):
    drawn = jax.random.normal(stream_key, dims, jnp.float32) * scale
    if len(shards) > 0:
        drawn = shard_levels(stream_key, dims, shards, -0.22, 0.18) * drawn
    return jnp.clip(drawn, min=-limit, max=limit).astype(kind)


def setup_inputs(seed: int = 0) -> dict:
    splits = jax.random.split(jax.random.key(seed), 4)
    grad_blocks = centred(splits[0], (NBLK, BLOCK, BLOCK), BLOCK ** -0.5, 0.5, ((0, 8), (2, 4)))
    owner_table = draw_owner_table(jax.random.fold_in(splits[3], 71), 0)
    prev_stats = draw_prev_stats(jax.random.fold_in(splits[3], 71), 0)
    return dict(grad_blocks=grad_blocks, owner_table=owner_table, prev_stats=prev_stats)


STAT_DECAY = 0.75
DAMPING = 0.03

def batch_product(first, second):
    return jnp.einsum('pij,pjk->pik', first, second, precision=lax.Precision.HIGHEST)

def newton_roots(matrices):
    width = matrices.shape[-1]
    identity = jnp.eye(width, dtype=jnp.float32)
    trace_val = jnp.trace(matrices, axis1=1, axis2=2)
    damped = matrices + DAMPING / width * trace_val[:, None, None] * identity
    norm_val = jnp.sqrt(lax.optimization_barrier(jnp.sum(damped * damped, axis=(1, 2))))
    root_mat = identity * (1.0 / jnp.sqrt(jnp.sqrt(norm_val)))[:, None, None]
    remainder = damped / norm_val[:, None, None]

    def refine(unused, state_pair):
        root_now, rest_now = state_pair
        factor = (5.0 * identity - rest_now) * 0.25
        root_now = batch_product(root_now, factor)
        square = batch_product(factor, factor)
        quartic = batch_product(square, square)
        return (root_now, batch_product(quartic, rest_now))
    root_mat, remainder = lax.fori_loop(0, ITERS, refine, (root_mat, remainder))
    return root_mat

def reference(grad_blocks, owner_table, prev_stats):
    grad_wide = grad_blocks.astype(jnp.float32)
    left_stat = jnp.einsum('bik,bjk->bij', grad_wide, grad_wide, precision=lax.Precision.HIGHEST)
    right_stat = jnp.einsum('bki,bkj->bij', grad_wide, grad_wide, precision=lax.Precision.HIGHEST)
    owners_hot = (owner_table[:, None] == jnp.arange(N_DP, dtype=jnp.int32)[None, :]).astype(jnp.int32)
    earlier = jnp.cumsum(owners_hot, axis=0) - owners_hot
    slot_rank = lax.optimization_barrier(jnp.sum(earlier * owners_hot, axis=1))
    slot_ids = (owner_table * CAP + slot_rank).astype(jnp.int32)
    previous = prev_stats[slot_ids]
    blended = STAT_DECAY * previous + (1.0 - STAT_DECAY) * jnp.stack([left_stat, right_stat], axis=1)
    roots = lax.map(newton_roots, blended)
    precond = jnp.einsum('bij,bjk->bik', roots[:, 0], grad_wide, precision=lax.Precision.HIGHEST)
    precond = jnp.einsum('bij,bjk->bik', precond, roots[:, 1], precision=lax.Precision.HIGHEST)
    spread = jnp.sqrt(lax.optimization_barrier(jnp.mean(precond * precond, axis=(1, 2))))
    update = (precond / spread[:, None, None]).astype(jnp.bfloat16)
    empty = jnp.zeros((N_DP * CAP, 2, BLOCK, BLOCK), jnp.float32)
    new_stats = empty.at[slot_ids].set(blended)
    inv_roots = empty.at[slot_ids].set(roots)
    return (update, new_stats, inv_roots)
```

```python
import functools

import jax
import jax.numpy as jnp
from jax import lax
from jax.experimental import pallas as pl
from jax.experimental.pallas import tpu as pltpu
from jax.sharding import PartitionSpec as P

ITERS = 16
STAT_DECAY = 0.75
DAMPING = 0.03
MESH = pl.DeviceIdType.MESH
BF = jnp.bfloat16
F32 = jnp.float32


def eye_of(n, dtype=F32):
    rows = lax.broadcasted_iota(jnp.int32, (n, n), 0)
    cols = lax.broadcasted_iota(jnp.int32, (n, n), 1)
    return (rows == cols).astype(F32).astype(dtype)


def pair(a):
    high = a.astype(BF)
    low = (a - high.astype(F32)).astype(BF)
    return jnp.concatenate([high, low], axis=1)


def twice(a):
    return jnp.concatenate([a, a], axis=0)


def product(left_pair, right_twice):
    out = jnp.dot(left_pair, right_twice, preferred_element_type=F32)
    width = out.shape[1] // 2
    return out[:, :width] + out[:, width:]


def total(a):
    return jnp.sum(jnp.sum(a, axis=1, keepdims=True), axis=0, keepdims=True)


def kernel(
    n_dp, n_mp, owner_ref, grad_ref, prev_hbm,
    upd_ref, nst_hbm, inv_hbm,
    rank_s, quarter, gbuf, hfull, prev, nst, roots, rest, usend, ubuf, obuf, rbuf,
    loc_sem, g_send, g_recv, m_send, m_recv, u_sem, r_sem, o_send, o_recv,
):
    blk_local, width, part = grad_ref.shape
    cap = prev.shape[0]
    half = cap // 2
    nblk = owner_ref.shape[0]
    me = lax.axis_index("dp")
    my = lax.axis_index("mp")
    mate = my + 1 - 2 * lax.rem(my, 2)
    first = half * lax.rem(my, 2)
    my_rows = pl.ds(pl.multiple_of(my * part, part), part)
    mate_rows = pl.ds(pl.multiple_of(mate * part, part), part)

    prev_in = pltpu.make_async_copy(prev_hbm, prev, loc_sem.at[0])
    prev_in.start()

    barrier = pltpu.get_barrier_semaphore()

    def greet(k, c):
        pl.semaphore_signal(
            barrier, inc=1, device_id={"dp": lax.rem(me + k, n_dp)}, device_id_type=MESH
        )
        return c

    lax.fori_loop(1, n_dp, greet, 0)
    for k in range(1, n_mp):
        pl.semaphore_signal(
            barrier, inc=1, device_id={"mp": lax.rem(my + k, n_mp)}, device_id_type=MESH
        )

    eye_bf = eye_of(width, BF)
    for j in range(blk_local):
        quarter[j] = lax.dot_general(
            grad_ref[j], eye_bf, (((0,), (0,)), ((), ())), preferred_element_type=F32
        ).astype(BF)
    gbuf[0] = quarter[...]

    def scan_table(b, carry):
        count = carry[0]
        mine = owner_ref[b] == me
        rank_s[b] = count
        picked = [
            jnp.where(mine & (count == r), b, carry[1 + r]) for r in range(cap)
        ]
        return (count + mine.astype(jnp.int32), *picked)

    found = lax.fori_loop(0, nblk, scan_table, (jnp.int32(0),) * (cap + 1))
    count, picks = found[0], found[1:]

    pl.semaphore_wait(barrier, n_dp - 1 + n_mp - 1)

    def spread_out(k, c):
        pltpu.make_async_remote_copy(
            src_ref=quarter, dst_ref=gbuf.at[k], send_sem=g_send, recv_sem=g_recv,
            device_id={"dp": lax.rem(me + k, n_dp)}, device_id_type=MESH,
        ).start()
        return c

    lax.fori_loop(1, n_dp, spread_out, 0)
    others = gbuf.at[pl.ds(1, n_dp - 1)]
    pltpu.make_async_copy(others, others, g_recv).wait()

    for r in range(cap):
        home = picks[r] // blk_local
        hfull[r, my_rows, :] = gbuf[
            lax.rem(me - home + n_dp, n_dp), picks[r] - home * blk_local
        ]
    mine_q = hfull.at[:, my_rows, :]
    swaps = []
    for k in range(1, n_mp):
        swap = pltpu.make_async_remote_copy(
            src_ref=mine_q, dst_ref=mine_q,
            send_sem=m_send.at[k - 1], recv_sem=m_recv.at[k - 1],
            device_id={"mp": lax.rem(my + k, n_mp)}, device_id_type=MESH,
        )
        swap.start()
        swaps.append(swap)
    prev_in.wait()
    pltpu.make_async_copy(others, others, g_send).wait()
    for k in range(1, n_mp):
        came = hfull.at[:, pl.ds(pl.multiple_of(lax.rem(my - k + n_mp, n_mp) * part, part), part), :]
        pltpu.make_async_copy(came, came, m_recv.at[k - 1]).wait()

    eye = eye_of(width)
    for r in range(cap):
        h = hfull[r]
        left = lax.dot_general(h, h, (((0,), (0,)), ((), ())), preferred_element_type=F32)
        right = lax.dot_general(h, h, (((1,), (1,)), ((), ())), preferred_element_type=F32)
        for side, stat in ((0, left), (1, right)):
            mix = STAT_DECAY * prev[r, side] + (1.0 - STAT_DECAY) * stat
            nst[r, side] = jnp.where(r < count, mix, 0.0)
            prev[r, side] = jnp.where(r < count, mix, eye)
    nst_out = pltpu.make_async_copy(nst, nst_hbm, loc_sem.at[1])
    nst_out.start()

    slots = [(first + i // 2, i % 2) for i in range(2 * half)]
    span = range(2 * half)
    for i in span:
        s = prev[slots[i]]
        a = s + (DAMPING / width) * total(s * eye) * eye
        c = jnp.sqrt(total(a * a))
        roots[slots[i]] = eye * (1.0 / jnp.sqrt(jnp.sqrt(c)))
        rest[i] = a * (1.0 / c)

    def refine(_, carry):
        ident = eye_of(width)
        xs = [roots[slots[i]] for i in span]
        ms = [rest[i] for i in span]
        ml = [pair(m) for m in ms]
        mr = [twice(m) for m in ml]
        out = [product(jnp.concatenate([ml[i], pair(xs[i])], axis=0), mr[i]) for i in span]
        sq = [
            ident * 1.5625 - ms[i] * 0.625 + out[i][:width] * 0.0625 for i in span
        ]
        for i in span:
            roots[slots[i]] = xs[i] * 1.25 - out[i][width:] * 0.25
        sl = [pair(s) for s in sq]
        us = [product(sl[i], mr[i]) for i in span]
        for i in span:
            rest[i] = product(pair(us[i]), twice(sl[i]))
        return carry

    lax.fori_loop(0, ITERS - 1, refine, 0)
    ms = [pair(rest[i]) for i in span]
    out = [product(pair(roots[slots[i]]), twice(ms[i])) for i in span]
    for i in span:
        roots[slots[i]] = roots[slots[i]] * 1.25 - out[i] * 0.25

    r0 = [pair(roots[slots[2 * i]]) for i in range(half)]
    r1 = [pair(roots[slots[2 * i + 1]]) for i in range(half)]
    mid = [
        jnp.dot(r1[i], twice(hfull[first + i]), preferred_element_type=F32)
        for i in range(half)
    ]
    pre = [product(pair(mid[i]), twice(r0[i])) for i in range(half)]
    for i in range(half):
        rms = jnp.sqrt(total(pre[i] * pre[i]) * (1.0 / (width * width)))
        rest[i] = pre[i] / rms
    for i in range(half):
        ubuf[first + i] = rest[i, my_rows, :].astype(BF)
        usend[i] = rest[i, mate_rows, :].astype(BF)
    u_swap = pltpu.make_async_remote_copy(
        src_ref=usend, dst_ref=ubuf.at[pl.ds(first, half)],
        send_sem=u_sem.at[0], recv_sem=u_sem.at[1],
        device_id={"mp": mate}, device_id_type=MESH,
    )
    u_swap.start()
    my_roots = roots.at[pl.ds(first, half)]
    r_swap = pltpu.make_async_remote_copy(
        src_ref=my_roots, dst_ref=my_roots,
        send_sem=r_sem.at[0], recv_sem=r_sem.at[1],
        device_id={"mp": mate}, device_id_type=MESH,
    )
    r_swap.start()
    theirs_u = ubuf.at[pl.ds(half - first, half)]
    pltpu.make_async_copy(theirs_u, theirs_u, u_sem.at[1]).wait()

    def address(k, c):
        home = lax.rem(me + k, n_dp)
        for j in range(blk_local):
            b = home * blk_local + j
            row = jnp.minimum(rank_s[b], cap - 1)
            obuf[k, j] = jnp.where(owner_ref[b] == me, ubuf[row], jnp.zeros((), BF))
        return c

    lax.fori_loop(0, n_dp, address, 0)
    rbuf[0] = obuf[0]

    def give_back(k, c):
        pltpu.make_async_remote_copy(
            src_ref=obuf.at[k], dst_ref=rbuf.at[k], send_sem=o_send, recv_sem=o_recv,
            device_id={"dp": lax.rem(me + k, n_dp)}, device_id_type=MESH,
        ).start()
        return c

    lax.fori_loop(1, n_dp, give_back, 0)

    theirs_r = roots.at[pl.ds(half - first, half)]
    pltpu.make_async_copy(theirs_r, theirs_r, r_sem.at[1]).wait()
    nst_out.wait()
    for r in range(cap):
        for side in range(2):
            nst[r, side] = jnp.where(r < count, roots[r, side], 0.0)
    inv_out = pltpu.make_async_copy(nst, inv_hbm, loc_sem.at[2])
    inv_out.start()

    back = rbuf.at[pl.ds(1, n_dp - 1)]
    pltpu.make_async_copy(back, back, o_recv).wait()
    for j in range(blk_local):
        owner = owner_ref[me * blk_local + j]
        got = rbuf[lax.rem(me - owner + n_dp, n_dp), j]
        upd_ref[j] = lax.dot_general(
            eye_bf, got, (((1,), (1,)), ((), ())), preferred_element_type=F32
        ).astype(BF)

    for swap in swaps:
        swap.wait_send()
    u_swap.wait_send()
    r_swap.wait_send()
    pltpu.make_async_copy(back, back, o_send).wait()
    inv_out.wait()


def solution(mesh):
    n_dp, n_mp = mesh.shape["dp"], mesh.shape["mp"]

    def per_device(grad_blocks, owner_table, prev_stats):
        blk_local, width, part = grad_blocks.shape
        cap = prev_stats.shape[0]
        vmem = pl.BlockSpec(memory_space=pltpu.VMEM)
        hbm = pl.BlockSpec(memory_space=pl.ANY)
        strip = (blk_local, part, width)
        dma = pltpu.SemaphoreType.DMA
        return pl.pallas_call(
            functools.partial(kernel, n_dp, n_mp),
            out_shape=(
                jax.ShapeDtypeStruct(grad_blocks.shape, BF),
                jax.ShapeDtypeStruct(prev_stats.shape, F32),
                jax.ShapeDtypeStruct(prev_stats.shape, F32),
            ),
            in_specs=[pl.BlockSpec(memory_space=pltpu.SMEM), vmem, hbm],
            out_specs=(vmem, hbm, hbm),
            scratch_shapes=[
                pltpu.SMEM((owner_table.shape[0],), jnp.int32),
                pltpu.VMEM(strip, BF),
                pltpu.VMEM((n_dp, *strip), BF),
                pltpu.VMEM((cap, width, width), BF),
                pltpu.VMEM(prev_stats.shape, F32),
                pltpu.VMEM(prev_stats.shape, F32),
                pltpu.VMEM(prev_stats.shape, F32),
                pltpu.VMEM((cap, width, width), F32),
                pltpu.VMEM((cap // 2, part, width), BF),
                pltpu.VMEM((cap, part, width), BF),
                pltpu.VMEM((n_dp, *strip), BF),
                pltpu.VMEM((n_dp, *strip), BF),
                dma((3,)), dma, dma, dma((n_mp - 1,)), dma((n_mp - 1,)),
                dma((2,)), dma((2,)), dma, dma,
            ],
            compiler_params=pltpu.CompilerParams(
                collective_id=0, has_side_effects=True, vmem_limit_bytes=40 << 20
            ),
        )(owner_table, grad_blocks, prev_stats)

    return jax.shard_map(
        per_device,
        mesh=mesh,
        in_specs=(P("dp", None, "mp"), P(), P("dp", None, None, None)),
        out_specs=(P("dp", None, "mp"), P("dp", None, None, None), P("dp", None, None, None)),
        check_vma=False,
    )
```

```python
import functools

import jax
import jax.numpy as jnp
from jax import lax
from jax.experimental import pallas as pl
from jax.experimental.pallas import tpu as pltpu
from jax.sharding import PartitionSpec as P

ITERS = 16
STAT_DECAY = 0.75
DAMPING = 0.03
MESH = pl.DeviceIdType.MESH
BF = jnp.bfloat16
F32 = jnp.float32


def eye_of(n, dtype=F32):
    rows = lax.broadcasted_iota(jnp.int32, (n, n), 0)
    cols = lax.broadcasted_iota(jnp.int32, (n, n), 1)
    return (rows == cols).astype(F32).astype(dtype)


def pair(a):
    high = a.astype(BF)
    low = (a - high.astype(F32)).astype(BF)
    return jnp.concatenate([high, low], axis=1)


def twice(a):
    return jnp.concatenate([a, a], axis=0)


def product(left_pair, right_twice):
    out = jnp.dot(left_pair, right_twice, preferred_element_type=F32)
    width = out.shape[1] // 2
    return out[:, :width] + out[:, width:]


def total(a):
    return jnp.sum(jnp.sum(a, axis=1, keepdims=True), axis=0, keepdims=True)


def kernel(
    n_dp, n_mp, owner_ref, grad_ref, prev_hbm,
    upd_ref, nst, inv,
    rank_s, gall, prev, roots, rest, usend, ubuf, obuf, rbuf,
    loc_sem, g_send, g_recv, m_send, m_recv, u_send, u_recv, r_send, r_recv, f_send, f_recv,
    o_send, o_recv,
):
    blk_local, part, width = grad_ref.shape
    cap = prev.shape[0]
    own = cap // n_mp
    nblk = owner_ref.shape[0]
    me = lax.axis_index("dp")
    my = lax.axis_index("mp")
    mate = my + 1 - 2 * lax.rem(my, 2)
    first = own * my
    low_half = me < n_dp // 2

    def rows_of(index):
        return pl.ds(pl.multiple_of(index * part, part), part)

    def slots_of(index):
        return pl.ds(index * own, own)

    def far_first(i):
        return jnp.where(low_half, n_dp - 1 - i, i)

    def offset(d):
        return lax.rem(d - me + n_dp, n_dp)

    def peer(k):
        return lax.rem(my + k, n_mp)

    prev_in = pltpu.make_async_copy(prev_hbm, prev, loc_sem)
    prev_in.start()

    barrier = pltpu.get_barrier_semaphore()

    def greet(k, c):
        pl.semaphore_signal(
            barrier, inc=1, device_id={"dp": lax.rem(me + k, n_dp)}, device_id_type=MESH
        )
        return c

    lax.fori_loop(1, n_dp, greet, 0)
    for k in range(1, n_mp):
        pl.semaphore_signal(barrier, inc=1, device_id={"mp": peer(k)}, device_id_type=MESH)

    my_rows = rows_of(my)
    gall[0, :, my_rows, :] = grad_ref[...]

    def scan_table(b, carry):
        count = carry[0]
        mine = owner_ref[b] == me
        rank_s[b] = count
        picked = [
            jnp.where(mine & (count == r), b, carry[1 + r]) for r in range(cap)
        ]
        return (count + mine.astype(jnp.int32), *picked)

    found = lax.fori_loop(0, nblk, scan_table, (jnp.int32(0),) * (cap + 1))
    count, picks = found[0], found[1:]

    pl.semaphore_wait(barrier, n_dp - 1 + n_mp - 1)

    def spread_out(i, c):
        d = far_first(i)

        @pl.when(d != me)
        def _():
            k = offset(d)
            pltpu.make_async_remote_copy(
                src_ref=grad_ref, dst_ref=gall.at[k, :, my_rows, :],
                send_sem=g_send, recv_sem=g_recv.at[k],
                device_id={"dp": d}, device_id_type=MESH,
            ).start()

        return c

    def pass_on(src, k):
        for j in range(1, n_mp):
            pltpu.make_async_remote_copy(
                src_ref=src, dst_ref=gall.at[k, :, my_rows, :],
                send_sem=m_send.at[j - 1], recv_sem=m_recv.at[j - 1],
                device_id={"mp": peer(j)}, device_id_type=MESH,
            ).start()

    lax.fori_loop(0, n_dp, spread_out, 0)
    pass_on(grad_ref, 0)

    def relay(i, c):
        d = far_first(n_dp - 1 - i)

        @pl.when(d != me)
        def _():
            k = lax.rem(me - d + n_dp, n_dp)
            strip = gall.at[k, :, my_rows, :]
            pltpu.make_async_copy(strip, strip, g_recv.at[k]).wait()
            pass_on(strip, k)

        return c

    lax.fori_loop(0, n_dp, relay, 0)
    prev_in.wait()
    for j in range(1, n_mp):
        came = gall.at[:, :, rows_of(lax.rem(my - j + n_mp, n_mp)), :]
        pltpu.make_async_copy(came, came, m_recv.at[j - 1]).wait()

    def block_of(r):
        home = picks[r] // blk_local
        return gall[lax.rem(me - home + n_dp, n_dp), picks[r] - home * blk_local]

    def pick_at(i):
        b = picks[i]
        for q in range(1, n_mp):
            b = jnp.where(my == q, picks[q * own + i], b)
        home = b // blk_local
        return lax.rem(me - home + n_dp, n_dp), b - home * blk_local

    spots = [pick_at(i) for i in range(own)]
    eye = eye_of(width)
    for r in range(cap):
        h = block_of(r)
        left = lax.dot_general(h, h, (((0,), (0,)), ((), ())), preferred_element_type=F32)
        right = lax.dot_general(h, h, (((1,), (1,)), ((), ())), preferred_element_type=F32)
        for side, stat in ((0, left), (1, right)):
            mix = STAT_DECAY * prev[r, side] + (1.0 - STAT_DECAY) * stat
            nst[r, side] = jnp.where(r < count, mix, 0.0)
            prev[r, side] = jnp.where(r < count, mix, eye)

    slots = [(first + i // 2, i % 2) for i in range(2 * own)]
    span = range(2 * own)
    for i in span:
        s = prev[slots[i]]
        a = s + (DAMPING / width) * total(s * eye) * eye
        c = jnp.sqrt(total(a * a))
        roots[slots[i]] = eye * (1.0 / jnp.sqrt(jnp.sqrt(c)))
        rest[i] = a * (1.0 / c)

    def refine(_, carry):
        ident = eye_of(width)
        xs = [roots[slots[i]] for i in span]
        ms = [rest[i] for i in span]
        ml = [pair(m) for m in ms]
        mr = [twice(m) for m in ml]
        out = [product(jnp.concatenate([ml[i], pair(xs[i])], axis=0), mr[i]) for i in span]
        sq = [
            ident * 1.5625 - ms[i] * 0.625 + out[i][:width] * 0.0625 for i in span
        ]
        for i in span:
            roots[slots[i]] = xs[i] * 1.25 - out[i][width:] * 0.25
        sl = [pair(s) for s in sq]
        us = [product(sl[i], mr[i]) for i in span]
        for i in span:
            rest[i] = product(pair(us[i]), twice(sl[i]))
        return carry

    lax.fori_loop(0, ITERS - 1, refine, 0)
    ms = [pair(rest[i]) for i in span]
    out = [product(pair(roots[slots[i]]), twice(ms[i])) for i in span]
    for i in span:
        roots[slots[i]] = roots[slots[i]] * 1.25 - out[i] * 0.25

    def root_copy(src_owner, to, sems, slot):
        part_of = roots.at[src_owner * own + slot]
        return pltpu.make_async_remote_copy(
            src_ref=part_of, dst_ref=part_of, send_sem=sems[0], recv_sem=sems[1],
            device_id={"mp": to}, device_id_type=MESH,
        )

    r0 = [pair(roots[slots[2 * i]]) for i in range(own)]
    r1 = [pair(roots[slots[2 * i + 1]]) for i in range(own)]
    mids = []
    for i in range(own):
        spot = spots[i]
        mids.append(jnp.dot(r1[i], twice(gall[spot[0], spot[1]]), preferred_element_type=F32))
    pre = [product(pair(mids[i]), twice(r0[i])) for i in range(own)]
    for i in range(own):
        rms = jnp.sqrt(total(pre[i] * pre[i]) * (1.0 / (width * width)))
        rest[i] = pre[i] / rms
    for i in range(own):
        for k in range(n_mp):
            rows = rest[i, rows_of(peer(k)), :].astype(BF)
            if k == 0:
                ubuf[first + i] = rows
            else:
                usend[k - 1, i] = rows
    u_swaps = []
    for k in range(1, n_mp):
        u_swaps.append(pltpu.make_async_remote_copy(
            src_ref=usend.at[k - 1], dst_ref=ubuf.at[slots_of(my)],
            send_sem=u_send.at[k - 1], recv_sem=u_recv.at[k - 1],
            device_id={"mp": peer(k)}, device_id_type=MESH,
        ))
        u_swaps[-1].start()
    root_swaps = []
    for i in range(own):
        for j in range(n_mp // 2):
            to = mate if j == 0 else peer(2 * j)
            root_swaps.append(root_copy(my, to, (r_send.at[j, i], r_recv.at[j, i]), i))
            root_swaps[-1].start()
    for k in range(1, n_mp):
        came = ubuf.at[slots_of(lax.rem(my - k + n_mp, n_mp))]
        pltpu.make_async_copy(came, came, u_recv.at[k - 1]).wait()

    def address(k, c):
        home = lax.rem(me + k, n_dp)
        for j in range(blk_local):
            b = home * blk_local + j
            row = jnp.minimum(rank_s[b], cap - 1)
            obuf[k, j] = jnp.where(owner_ref[b] == me, ubuf[row], jnp.zeros((), BF))
        return c

    lax.fori_loop(0, n_dp, address, 0)
    rbuf[0] = obuf[0]

    def give_back(i, c):
        d = far_first(i)

        @pl.when(d != me)
        def _():
            k = offset(d)
            pltpu.make_async_remote_copy(
                src_ref=obuf.at[k], dst_ref=rbuf.at[k], send_sem=o_send, recv_sem=o_recv,
                device_id={"dp": d}, device_id_type=MESH,
            ).start()

        return c

    lax.fori_loop(0, n_dp, give_back, 0)

    for i in range(own):
        for j in range(1, n_mp // 2):
            source = lax.rem(my - 2 * j + n_mp, n_mp)
            came = roots.at[source * own + i]
            pltpu.make_async_copy(came, came, r_recv.at[j, i]).wait()
            root_swaps.append(root_copy(source, mate, (f_send.at[j - 1, i], f_recv.at[j - 1, i]), i))
            root_swaps[-1].start()
    for i in range(own):
        for j in range(n_mp // 2):
            source = lax.rem(mate - 2 * j + n_mp, n_mp)
            came = roots.at[source * own + i]
            sem = r_recv.at[0, i] if j == 0 else f_recv.at[j - 1, i]
            pltpu.make_async_copy(came, came, sem).wait()
    for r in range(cap):
        for side in range(2):
            inv[r, side] = jnp.where(r < count, roots[r, side], 0.0)

    back = rbuf.at[pl.ds(1, n_dp - 1)]
    pltpu.make_async_copy(back, back, o_recv).wait()
    for j in range(blk_local):
        owner = owner_ref[me * blk_local + j]
        got = rbuf[lax.rem(me - owner + n_dp, n_dp), j]
        upd_ref[j] = got

    for swap in u_swaps + root_swaps:
        swap.wait_send()
    others = gall.at[pl.ds(1, n_dp - 1), :, my_rows, :]
    pltpu.make_async_copy(others, others, g_send).wait()
    for j in range(1, n_mp):
        sent = gall.at[:, :, my_rows, :]
        pltpu.make_async_copy(sent, sent, m_send.at[j - 1]).wait()
    pltpu.make_async_copy(back, back, o_send).wait()


def write_out(upd, nst, inv, upd_out, nst_out, inv_out, sems):
    copies = [
        pltpu.make_async_copy(src, dst, sems.at[i])
        for i, (src, dst) in enumerate(((nst, nst_out), (inv, inv_out), (upd, upd_out)))
    ]
    for copy in copies:
        copy.start()
    for copy in copies:
        copy.wait()


def solution(mesh):
    n_dp, n_mp = mesh.shape["dp"], mesh.shape["mp"]

    def per_device(grad_blocks, owner_table, prev_stats):
        strips = jnp.swapaxes(grad_blocks, 1, 2)
        blk_local, part, width = strips.shape
        cap = prev_stats.shape[0]
        own = cap // n_mp
        vmem = pl.BlockSpec(memory_space=pltpu.VMEM)
        hbm = pl.BlockSpec(memory_space=pltpu.HBM)
        strip = strips.shape
        dma = pltpu.SemaphoreType.DMA
        shapes = (
            jax.ShapeDtypeStruct(strip, BF),
            jax.ShapeDtypeStruct(prev_stats.shape, F32),
            jax.ShapeDtypeStruct(prev_stats.shape, F32),
        )
        held = pl.pallas_call(
            functools.partial(kernel, n_dp, n_mp),
            out_shape=shapes,
            in_specs=[pl.BlockSpec(memory_space=pltpu.SMEM), vmem, hbm],
            out_specs=(vmem, vmem, vmem),
            scratch_shapes=[
                pltpu.SMEM((owner_table.shape[0],), jnp.int32),
                pltpu.VMEM((n_dp, blk_local, width, width), BF),
                pltpu.VMEM(prev_stats.shape, F32),
                pltpu.VMEM(prev_stats.shape, F32),
                pltpu.VMEM((2 * own, width, width), F32),
                pltpu.VMEM((n_mp - 1, own, part, width), BF),
                pltpu.VMEM((cap, part, width), BF),
                pltpu.VMEM((n_dp, *strip), BF),
                pltpu.VMEM((n_dp, *strip), BF),
                dma, dma, dma((n_dp,)), dma((n_mp - 1,)), dma((n_mp - 1,)),
                dma((n_mp - 1,)), dma((n_mp - 1,)),
                dma((n_mp // 2, own)), dma((n_mp // 2, own)),
                dma((n_mp // 2, own)), dma((n_mp // 2, own)), dma, dma,
            ],
            compiler_params=pltpu.CompilerParams(
                collective_id=0, has_side_effects=True, vmem_limit_bytes=32 << 20
            ),
        )(owner_table, strips, prev_stats)
        update, new_stats, inv_roots = pl.pallas_call(
            write_out,
            out_shape=shapes,
            in_specs=[pl.BlockSpec(memory_space=pl.ANY)] * 3,
            out_specs=(hbm, hbm, hbm),
            scratch_shapes=[dma((3,))],
            compiler_params=pltpu.CompilerParams(vmem_limit_bytes=1 << 20),
        )(*held)
        return jnp.swapaxes(update, 1, 2), new_stats, inv_roots

    return jax.shard_map(
        per_device,
        mesh=mesh,
        in_specs=(P("dp", None, "mp"), P(), P("dp", None, None, None)),
        out_specs=(P("dp", None, "mp"), P("dp", None, None, None), P("dp", None, None, None)),
        check_vma=False,
    )
```

```python
import functools

import jax
import jax.numpy as jnp
from jax import lax
from jax.experimental import pallas as pl
from jax.experimental.pallas import tpu as pltpu
from jax.sharding import PartitionSpec as P

ITERS = 16
STAT_DECAY = 0.75
DAMPING = 0.03
MESH = pl.DeviceIdType.MESH
BF = jnp.bfloat16
F32 = jnp.float32


def eye_of(n, dtype=F32):
    rows = lax.broadcasted_iota(jnp.int32, (n, n), 0)
    cols = lax.broadcasted_iota(jnp.int32, (n, n), 1)
    return (rows == cols).astype(F32).astype(dtype)


def pair(a):
    high = a.astype(BF)
    low = (a - high.astype(F32)).astype(BF)
    return jnp.concatenate([high, low], axis=1)


def twice(a):
    return jnp.concatenate([a, a], axis=0)


def product(left_pair, right_twice):
    out = jnp.dot(left_pair, right_twice, preferred_element_type=F32)
    width = out.shape[1] // 2
    return out[:, :width] + out[:, width:]


def total(a):
    return jnp.sum(jnp.sum(a, axis=1, keepdims=True), axis=0, keepdims=True)


def kernel(
    n_dp, n_mp, owner_ref, grad_ref, prev_hbm,
    upd_ref, nst, inv,
    rank_s, gbuf, hfull, hown, prev, roots, rest, usend, ubuf, obuf, rbuf,
    loc_sem, g_send, g_recv, m_send, m_recv, b_send, b_recv, u_send, u_recv, r_send, r_recv, f_send, f_recv,
    o_send, o_recv,
):
    blk_local, part, width = grad_ref.shape
    cap = prev.shape[0]
    own = cap // n_mp
    nblk = owner_ref.shape[0]
    me = lax.axis_index("dp")
    my = lax.axis_index("mp")
    mate = my + 1 - 2 * lax.rem(my, 2)
    first = own * my
    low_half = me < n_dp // 2

    def rows_of(index):
        return pl.ds(pl.multiple_of(index * part, part), part)

    def slots_of(index):
        return pl.ds(index * own, own)

    def far_first(i):
        return jnp.where(low_half, n_dp - 1 - i, i)

    def offset(d):
        return lax.rem(d - me + n_dp, n_dp)

    def peer(k):
        return lax.rem(my + k, n_mp)

    prev_in = pltpu.make_async_copy(prev_hbm, prev, loc_sem)
    prev_in.start()

    barrier = pltpu.get_barrier_semaphore()

    def greet(k, c):
        pl.semaphore_signal(
            barrier, inc=1, device_id={"dp": lax.rem(me + k, n_dp)}, device_id_type=MESH
        )
        return c

    lax.fori_loop(1, n_dp, greet, 0)
    for k in range(1, n_mp):
        pl.semaphore_signal(barrier, inc=1, device_id={"mp": peer(k)}, device_id_type=MESH)

    my_rows = rows_of(my)
    gbuf[0] = grad_ref[...]

    def scan_table(b, carry):
        count = carry[0]
        mine = owner_ref[b] == me
        rank_s[b] = count
        picked = [
            jnp.where(mine & (count == r), b, carry[1 + r]) for r in range(cap)
        ]
        return (count + mine.astype(jnp.int32), *picked)

    found = lax.fori_loop(0, nblk, scan_table, (jnp.int32(0),) * (cap + 1))
    count, picks = found[0], found[1:]

    pl.semaphore_wait(barrier, n_dp - 1 + n_mp - 1)

    def spread_out(i, c):
        d = far_first(i)

        @pl.when(d != me)
        def _():
            k = offset(d)
            pltpu.make_async_remote_copy(
                src_ref=grad_ref, dst_ref=gbuf.at[k], send_sem=g_send, recv_sem=g_recv,
                device_id={"dp": d}, device_id_type=MESH,
            ).start()

        return c

    lax.fori_loop(0, n_dp, spread_out, 0)
    others = gbuf.at[pl.ds(1, n_dp - 1)]
    pltpu.make_async_copy(others, others, g_recv).wait()

    for r in range(cap):
        home = picks[r] // blk_local
        hfull[r, my_rows, :] = gbuf[
            lax.rem(me - home + n_dp, n_dp), picks[r] - home * blk_local
        ]
    swaps = []
    for sems, whole in (((m_send, m_recv), False), ((b_send, b_recv), True)):
        for k in range(1, n_mp):
            src = hfull.at[:, my_rows, :] if whole else hfull.at[slots_of(peer(k)), my_rows, :]
            swaps.append(pltpu.make_async_remote_copy(
                src_ref=src, dst_ref=src if whole else hown.at[:, my_rows, :],
                send_sem=sems[0].at[k - 1], recv_sem=sems[1].at[k - 1],
                device_id={"mp": peer(k)}, device_id_type=MESH,
            ))
            swaps[-1].start()
    hown[:, my_rows, :] = hfull[slots_of(my), my_rows, :]
    prev_in.wait()

    def collect(buffer, sems):
        for k in range(1, n_mp):
            came = buffer.at[:, rows_of(lax.rem(my - k + n_mp, n_mp)), :]
            pltpu.make_async_copy(came, came, sems.at[k - 1]).wait()

    def blend(h, slot):
        left = lax.dot_general(h, h, (((0,), (0,)), ((), ())), preferred_element_type=F32)
        right = lax.dot_general(h, h, (((1,), (1,)), ((), ())), preferred_element_type=F32)
        return [
            STAT_DECAY * prev[slot, side] + (1.0 - STAT_DECAY) * stat
            for side, stat in ((0, left), (1, right))
        ]

    collect(hown, m_recv)
    eye = eye_of(width)
    slots = [(first + i // 2, i % 2) for i in range(2 * own)]
    span = range(2 * own)
    mixes = [m for i in range(own) for m in blend(hown[i], first + i)]
    for i in span:
        s = jnp.where(slots[i][0] < count, mixes[i], eye)
        a = s + (DAMPING / width) * total(s * eye) * eye
        c = jnp.sqrt(total(a * a))
        roots[slots[i]] = eye * (1.0 / jnp.sqrt(jnp.sqrt(c)))
        rest[i] = a * (1.0 / c)

    def refine(_, carry):
        ident = eye_of(width)
        xs = [roots[slots[i]] for i in span]
        ms = [rest[i] for i in span]
        ml = [pair(m) for m in ms]
        mr = [twice(m) for m in ml]
        out = [product(jnp.concatenate([ml[i], pair(xs[i])], axis=0), mr[i]) for i in span]
        sq = [
            ident * 1.5625 - ms[i] * 0.625 + out[i][:width] * 0.0625 for i in span
        ]
        for i in span:
            roots[slots[i]] = xs[i] * 1.25 - out[i][width:] * 0.25
        sl = [pair(s) for s in sq]
        us = [product(sl[i], mr[i]) for i in span]
        for i in span:
            rest[i] = product(pair(us[i]), twice(sl[i]))
        return carry

    lax.fori_loop(0, ITERS - 1, refine, 0)
    ms = [pair(rest[i]) for i in span]
    out = [product(pair(roots[slots[i]]), twice(ms[i])) for i in span]
    for i in span:
        roots[slots[i]] = roots[slots[i]] * 1.25 - out[i] * 0.25

    def root_copy(src_owner, to, sems, slot):
        part_of = roots.at[src_owner * own + slot]
        return pltpu.make_async_remote_copy(
            src_ref=part_of, dst_ref=part_of, send_sem=sems[0], recv_sem=sems[1],
            device_id={"mp": to}, device_id_type=MESH,
        )

    r0 = [pair(roots[slots[2 * i]]) for i in range(own)]
    r1 = [pair(roots[slots[2 * i + 1]]) for i in range(own)]
    mids = []
    for i in range(own):
        mids.append(jnp.dot(r1[i], twice(hown[i]), preferred_element_type=F32))
    pre = [product(pair(mids[i]), twice(r0[i])) for i in range(own)]
    for i in range(own):
        rms = jnp.sqrt(total(pre[i] * pre[i]) * (1.0 / (width * width)))
        rest[i] = pre[i] / rms
    for i in range(own):
        for k in range(n_mp):
            rows = rest[i, rows_of(peer(k)), :].astype(BF)
            if k == 0:
                ubuf[first + i] = rows
            else:
                usend[k - 1, i] = rows
    u_swaps = []
    for k in range(1, n_mp):
        u_swaps.append(pltpu.make_async_remote_copy(
            src_ref=usend.at[k - 1], dst_ref=ubuf.at[slots_of(my)],
            send_sem=u_send.at[k - 1], recv_sem=u_recv.at[k - 1],
            device_id={"mp": peer(k)}, device_id_type=MESH,
        ))
        u_swaps[-1].start()
    root_swaps = []
    for i in range(own):
        for j in range(n_mp // 2):
            to = mate if j == 0 else peer(2 * j)
            root_swaps.append(root_copy(my, to, (r_send.at[j, i], r_recv.at[j, i]), i))
            root_swaps[-1].start()
    for k in range(1, n_mp):
        came = ubuf.at[slots_of(lax.rem(my - k + n_mp, n_mp))]
        pltpu.make_async_copy(came, came, u_recv.at[k - 1]).wait()

    def address(k, c):
        home = lax.rem(me + k, n_dp)
        for j in range(blk_local):
            b = home * blk_local + j
            row = jnp.minimum(rank_s[b], cap - 1)
            obuf[k, j] = jnp.where(owner_ref[b] == me, ubuf[row], jnp.zeros((), BF))
        return c

    lax.fori_loop(0, n_dp, address, 0)
    rbuf[0] = obuf[0]

    def give_back(i, c):
        d = far_first(i)

        @pl.when(d != me)
        def _():
            k = offset(d)
            pltpu.make_async_remote_copy(
                src_ref=obuf.at[k], dst_ref=rbuf.at[k], send_sem=o_send, recv_sem=o_recv,
                device_id={"dp": d}, device_id_type=MESH,
            ).start()

        return c

    lax.fori_loop(0, n_dp, give_back, 0)

    collect(hfull, b_recv)
    for r in range(cap):
        for side, mix in enumerate(blend(hfull[r], r)):
            nst[r, side] = jnp.where(r < count, mix, 0.0)

    for i in range(own):
        for j in range(1, n_mp // 2):
            source = lax.rem(my - 2 * j + n_mp, n_mp)
            came = roots.at[source * own + i]
            pltpu.make_async_copy(came, came, r_recv.at[j, i]).wait()
            root_swaps.append(root_copy(source, mate, (f_send.at[j - 1, i], f_recv.at[j - 1, i]), i))
            root_swaps[-1].start()
    for i in range(own):
        for j in range(n_mp // 2):
            source = lax.rem(mate - 2 * j + n_mp, n_mp)
            came = roots.at[source * own + i]
            sem = r_recv.at[0, i] if j == 0 else f_recv.at[j - 1, i]
            pltpu.make_async_copy(came, came, sem).wait()
    for r in range(cap):
        for side in range(2):
            inv[r, side] = jnp.where(r < count, roots[r, side], 0.0)

    back = rbuf.at[pl.ds(1, n_dp - 1)]
    pltpu.make_async_copy(back, back, o_recv).wait()
    for j in range(blk_local):
        owner = owner_ref[me * blk_local + j]
        got = rbuf[lax.rem(me - owner + n_dp, n_dp), j]
        upd_ref[j] = got

    for swap in swaps + u_swaps + root_swaps:
        swap.wait_send()
    pltpu.make_async_copy(others, others, g_send).wait()
    pltpu.make_async_copy(back, back, o_send).wait()


def write_out(upd, nst, inv, upd_out, nst_out, inv_out, sems):
    copies = [
        pltpu.make_async_copy(src, dst, sems.at[i])
        for i, (src, dst) in enumerate(((nst, nst_out), (inv, inv_out), (upd, upd_out)))
    ]
    for copy in copies:
        copy.start()
    for copy in copies:
        copy.wait()


def solution(mesh):
    n_dp, n_mp = mesh.shape["dp"], mesh.shape["mp"]

    def per_device(grad_blocks, owner_table, prev_stats):
        strips = jnp.swapaxes(grad_blocks, 1, 2)
        blk_local, part, width = strips.shape
        cap = prev_stats.shape[0]
        own = cap // n_mp
        vmem = pl.BlockSpec(memory_space=pltpu.VMEM)
        hbm = pl.BlockSpec(memory_space=pltpu.HBM)
        strip = strips.shape
        dma = pltpu.SemaphoreType.DMA
        shapes = (
            jax.ShapeDtypeStruct(strip, BF),
            jax.ShapeDtypeStruct(prev_stats.shape, F32),
            jax.ShapeDtypeStruct(prev_stats.shape, F32),
        )
        held = pl.pallas_call(
            functools.partial(kernel, n_dp, n_mp),
            out_shape=shapes,
            in_specs=[pl.BlockSpec(memory_space=pltpu.SMEM), vmem, hbm],
            out_specs=(vmem, vmem, vmem),
            scratch_shapes=[
                pltpu.SMEM((owner_table.shape[0],), jnp.int32),
                pltpu.VMEM((n_dp, *strip), BF),
                pltpu.VMEM((cap, width, width), BF),
                pltpu.VMEM((own, width, width), BF),
                pltpu.VMEM(prev_stats.shape, F32),
                pltpu.VMEM(prev_stats.shape, F32),
                pltpu.VMEM((2 * own, width, width), F32),
                pltpu.VMEM((n_mp - 1, own, part, width), BF),
                pltpu.VMEM((cap, part, width), BF),
                pltpu.VMEM((n_dp, *strip), BF),
                pltpu.VMEM((n_dp, *strip), BF),
                dma, dma, dma, dma((n_mp - 1,)), dma((n_mp - 1,)),
                dma((n_mp - 1,)), dma((n_mp - 1,)),
                dma((n_mp - 1,)), dma((n_mp - 1,)),
                dma((n_mp // 2, own)), dma((n_mp // 2, own)),
                dma((n_mp // 2, own)), dma((n_mp // 2, own)), dma, dma,
            ],
            compiler_params=pltpu.CompilerParams(
                collective_id=0, has_side_effects=True, vmem_limit_bytes=32 << 20
            ),
        )(owner_table, strips, prev_stats)
        update, new_stats, inv_roots = pl.pallas_call(
            write_out,
            out_shape=shapes,
            in_specs=[pl.BlockSpec(memory_space=pl.ANY)] * 3,
            out_specs=(hbm, hbm, hbm),
            scratch_shapes=[dma((3,))],
            compiler_params=pltpu.CompilerParams(vmem_limit_bytes=1 << 20),
        )(*held)
        return jnp.swapaxes(update, 1, 2), new_stats, inv_roots

    return jax.shard_map(
        per_device,
        mesh=mesh,
        in_specs=(P("dp", None, "mp"), P(), P("dp", None, None, None)),
        out_specs=(P("dp", None, "mp"), P("dp", None, None, None), P("dp", None, None, None)),
        check_vma=False,
    )
```

```python
import functools

import jax
import jax.numpy as jnp
from jax import lax
from jax.experimental import pallas as pl
from jax.experimental.pallas import tpu as pltpu
from jax.sharding import PartitionSpec as P

ITERS = 16
STAT_DECAY = 0.75
DAMPING = 0.03
MESH = pl.DeviceIdType.MESH
BF = jnp.bfloat16
F32 = jnp.float32


def eye_of(n, dtype=F32):
    rows = lax.broadcasted_iota(jnp.int32, (n, n), 0)
    cols = lax.broadcasted_iota(jnp.int32, (n, n), 1)
    return (rows == cols).astype(F32).astype(dtype)


def pair(a):
    high = a.astype(BF)
    low = (a - high.astype(F32)).astype(BF)
    return jnp.concatenate([high, low], axis=1)


def twice(a):
    return jnp.concatenate([a, a], axis=0)


def product(left_pair, right_twice):
    out = jnp.dot(left_pair, right_twice, preferred_element_type=F32)
    width = out.shape[1] // 2
    return out[:, :width] + out[:, width:]


def total(a):
    return jnp.sum(jnp.sum(a, axis=1, keepdims=True), axis=0, keepdims=True)


def kernel(
    n_dp, n_mp, owner_ref, grad_ref, prev_hbm,
    upd_ref, nst, inv,
    rank_s, gbuf, hfull, hown, prev, roots, rest, usend, ubuf, obuf, rbuf,
    loc_sem, g_send, g_recv, m_send, m_recv, b_send, b_recv, u_send, u_recv, r_send, r_recv, f_send, f_recv,
    o_send, o_recv,
):
    blk_local, part, width = grad_ref.shape
    cap = prev.shape[0]
    own = cap // n_mp
    nblk = owner_ref.shape[0]
    me = lax.axis_index("dp")
    my = lax.axis_index("mp")
    mate = my + 1 - 2 * lax.rem(my, 2)
    first = own * my
    low_half = me < n_dp // 2

    def rows_of(index):
        return pl.ds(pl.multiple_of(index * part, part), part)

    def slots_of(index):
        return pl.ds(index * own, own)

    def far_first(i):
        return jnp.where(low_half, n_dp - 1 - i, i)

    def offset(d):
        return lax.rem(d - me + n_dp, n_dp)

    def peer(k):
        return lax.rem(my + k, n_mp)

    prev_in = pltpu.make_async_copy(prev_hbm, prev, loc_sem)
    prev_in.start()

    barrier = pltpu.get_barrier_semaphore()

    def greet(k, c):
        pl.semaphore_signal(
            barrier, inc=1, device_id={"dp": lax.rem(me + k, n_dp)}, device_id_type=MESH
        )
        return c

    lax.fori_loop(1, n_dp, greet, 0)
    for k in range(1, n_mp):
        pl.semaphore_signal(barrier, inc=1, device_id={"mp": peer(k)}, device_id_type=MESH)

    my_rows = rows_of(my)
    gbuf[0] = grad_ref[...]

    def scan_table(b, carry):
        count = carry[0]
        mine = owner_ref[b] == me
        rank_s[b] = count
        picked = [
            jnp.where(mine & (count == r), b, carry[1 + r]) for r in range(cap)
        ]
        return (count + mine.astype(jnp.int32), *picked)

    found = lax.fori_loop(0, nblk, scan_table, (jnp.int32(0),) * (cap + 1))
    count, picks = found[0], found[1:]

    pl.semaphore_wait(barrier, n_dp - 1 + n_mp - 1)

    def spread_out(i, c):
        d = far_first(i)

        @pl.when(d != me)
        def _():
            k = offset(d)
            pltpu.make_async_remote_copy(
                src_ref=grad_ref, dst_ref=gbuf.at[k], send_sem=g_send, recv_sem=g_recv,
                device_id={"dp": d}, device_id_type=MESH,
            ).start()

        return c

    lax.fori_loop(0, n_dp, spread_out, 0)
    others = gbuf.at[pl.ds(1, n_dp - 1)]
    pltpu.make_async_copy(others, others, g_recv).wait()

    for r in range(cap):
        home = picks[r] // blk_local
        hfull[r, my_rows, :] = gbuf[
            lax.rem(me - home + n_dp, n_dp), picks[r] - home * blk_local
        ]
    swaps = []
    for sems, whole in (((m_send, m_recv), False), ((b_send, b_recv), True)):
        for k in range(1, n_mp):
            src = hfull.at[:, my_rows, :] if whole else hfull.at[slots_of(peer(k)), my_rows, :]
            swaps.append(pltpu.make_async_remote_copy(
                src_ref=src, dst_ref=src if whole else hown.at[:, my_rows, :],
                send_sem=sems[0].at[k - 1], recv_sem=sems[1].at[k - 1],
                device_id={"mp": peer(k)}, device_id_type=MESH,
            ))
            swaps[-1].start()
    hown[:, my_rows, :] = hfull[slots_of(my), my_rows, :]
    prev_in.wait()

    def collect(buffer, sems):
        for k in range(1, n_mp):
            came = buffer.at[:, rows_of(lax.rem(my - k + n_mp, n_mp)), :]
            pltpu.make_async_copy(came, came, sems.at[k - 1]).wait()

    def blend(h, slot):
        left = lax.dot_general(h, h, (((0,), (0,)), ((), ())), preferred_element_type=F32)
        right = lax.dot_general(h, h, (((1,), (1,)), ((), ())), preferred_element_type=F32)
        return [
            STAT_DECAY * prev[slot, side] + (1.0 - STAT_DECAY) * stat
            for side, stat in ((0, left), (1, right))
        ]

    collect(hown, m_recv)
    eye = eye_of(width)
    slots = [(first + i // 2, i % 2) for i in range(2 * own)]
    span = range(2 * own)
    mixes = [m for i in range(own) for m in blend(hown[i], first + i)]
    for i in span:
        s = jnp.where(slots[i][0] < count, mixes[i], eye)
        a = s + (DAMPING / width) * total(s * eye) * eye
        c = jnp.sqrt(total(a * a))
        roots[slots[i]] = eye * (1.0 / jnp.sqrt(jnp.sqrt(c)))
        rest[i] = a * (1.0 / c)

    def refine(_, carry):
        ident = eye_of(width)
        xs = [roots[slots[i]] for i in span]
        ms = [rest[i] for i in span]
        ml = [pair(m) for m in ms]
        mr = [twice(m) for m in ml]
        out = [product(ml[i], mr[i]) for i in span]
        sq = [
            ident * 1.5625 - ms[i] * 0.625 + out[i] * 0.0625 for i in span
        ]
        sl = [pair(s) for s in sq]
        us = [product(sl[i], mr[i]) for i in span]
        xm = [product(pair(xs[i]), mr[i]) for i in span]
        for i in span:
            roots[slots[i]] = xs[i] * 1.25 - xm[i] * 0.25
        for i in span:
            rest[i] = product(pair(us[i]), twice(sl[i]))
        return carry

    lax.fori_loop(0, ITERS - 1, refine, 0, unroll=3)
    ms = [pair(rest[i]) for i in span]
    out = [product(pair(roots[slots[i]]), twice(ms[i])) for i in span]
    for i in span:
        roots[slots[i]] = roots[slots[i]] * 1.25 - out[i] * 0.25

    def root_copy(src_owner, to, sems, slot):
        part_of = roots.at[src_owner * own + slot]
        return pltpu.make_async_remote_copy(
            src_ref=part_of, dst_ref=part_of, send_sem=sems[0], recv_sem=sems[1],
            device_id={"mp": to}, device_id_type=MESH,
        )

    r0 = [pair(roots[slots[2 * i]]) for i in range(own)]
    r1 = [pair(roots[slots[2 * i + 1]]) for i in range(own)]
    mids = []
    for i in range(own):
        mids.append(jnp.dot(r1[i], twice(hown[i]), preferred_element_type=F32))
    pre = [product(pair(mids[i]), twice(r0[i])) for i in range(own)]
    for i in range(own):
        rms = jnp.sqrt(total(pre[i] * pre[i]) * (1.0 / (width * width)))
        rest[i] = pre[i] / rms
    for i in range(own):
        for k in range(n_mp):
            rows = rest[i, rows_of(peer(k)), :].astype(BF)
            if k == 0:
                ubuf[first + i] = rows
            else:
                usend[k - 1, i] = rows
    u_swaps = []
    for k in range(1, n_mp):
        u_swaps.append(pltpu.make_async_remote_copy(
            src_ref=usend.at[k - 1], dst_ref=ubuf.at[slots_of(my)],
            send_sem=u_send.at[k - 1], recv_sem=u_recv.at[k - 1],
            device_id={"mp": peer(k)}, device_id_type=MESH,
        ))
        u_swaps[-1].start()
    root_swaps = []
    for i in range(own):
        for j in range(n_mp // 2):
            to = mate if j == 0 else peer(2 * j)
            root_swaps.append(root_copy(my, to, (r_send.at[j, i], r_recv.at[j, i]), i))
            root_swaps[-1].start()
    for k in range(1, n_mp):
        came = ubuf.at[slots_of(lax.rem(my - k + n_mp, n_mp))]
        pltpu.make_async_copy(came, came, u_recv.at[k - 1]).wait()

    def address(k, c):
        home = lax.rem(me + k, n_dp)
        for j in range(blk_local):
            b = home * blk_local + j
            row = jnp.minimum(rank_s[b], cap - 1)
            obuf[k, j] = jnp.where(owner_ref[b] == me, ubuf[row], jnp.zeros((), BF))
        return c

    lax.fori_loop(0, n_dp, address, 0)
    rbuf[0] = obuf[0]

    def give_back(i, c):
        d = far_first(i)

        @pl.when(d != me)
        def _():
            k = offset(d)
            pltpu.make_async_remote_copy(
                src_ref=obuf.at[k], dst_ref=rbuf.at[k], send_sem=o_send, recv_sem=o_recv,
                device_id={"dp": d}, device_id_type=MESH,
            ).start()

        return c

    lax.fori_loop(0, n_dp, give_back, 0)

    collect(hfull, b_recv)
    for r in range(cap):
        for side, mix in enumerate(blend(hfull[r], r)):
            nst[r, side] = jnp.where(r < count, mix, 0.0)

    for i in range(own):
        for j in range(1, n_mp // 2):
            source = lax.rem(my - 2 * j + n_mp, n_mp)
            came = roots.at[source * own + i]
            pltpu.make_async_copy(came, came, r_recv.at[j, i]).wait()
            root_swaps.append(root_copy(source, mate, (f_send.at[j - 1, i], f_recv.at[j - 1, i]), i))
            root_swaps[-1].start()
    for i in range(own):
        for j in range(n_mp // 2):
            source = lax.rem(mate - 2 * j + n_mp, n_mp)
            came = roots.at[source * own + i]
            sem = r_recv.at[0, i] if j == 0 else f_recv.at[j - 1, i]
            pltpu.make_async_copy(came, came, sem).wait()
    for r in range(cap):
        for side in range(2):
            inv[r, side] = jnp.where(r < count, roots[r, side], 0.0)

    back = rbuf.at[pl.ds(1, n_dp - 1)]
    pltpu.make_async_copy(back, back, o_recv).wait()
    for j in range(blk_local):
        owner = owner_ref[me * blk_local + j]
        got = rbuf[lax.rem(me - owner + n_dp, n_dp), j]
        upd_ref[j] = got

    for swap in swaps + u_swaps + root_swaps:
        swap.wait_send()
    pltpu.make_async_copy(others, others, g_send).wait()
    pltpu.make_async_copy(back, back, o_send).wait()


def write_out(upd, nst, inv, upd_out, nst_out, inv_out, sems):
    copies = [
        pltpu.make_async_copy(src, dst, sems.at[i])
        for i, (src, dst) in enumerate(((nst, nst_out), (inv, inv_out), (upd, upd_out)))
    ]
    for copy in copies:
        copy.start()
    for copy in copies:
        copy.wait()


def solution(mesh):
    n_dp, n_mp = mesh.shape["dp"], mesh.shape["mp"]

    def per_device(grad_blocks, owner_table, prev_stats):
        strips = jnp.swapaxes(grad_blocks, 1, 2)
        blk_local, part, width = strips.shape
        cap = prev_stats.shape[0]
        own = cap // n_mp
        vmem = pl.BlockSpec(memory_space=pltpu.VMEM)
        hbm = pl.BlockSpec(memory_space=pltpu.HBM)
        strip = strips.shape
        dma = pltpu.SemaphoreType.DMA
        shapes = (
            jax.ShapeDtypeStruct(strip, BF),
            jax.ShapeDtypeStruct(prev_stats.shape, F32),
            jax.ShapeDtypeStruct(prev_stats.shape, F32),
        )
        held = pl.pallas_call(
            functools.partial(kernel, n_dp, n_mp),
            out_shape=shapes,
            in_specs=[pl.BlockSpec(memory_space=pltpu.SMEM), vmem, hbm],
            out_specs=(vmem, vmem, vmem),
            scratch_shapes=[
                pltpu.SMEM((owner_table.shape[0],), jnp.int32),
                pltpu.VMEM((n_dp, *strip), BF),
                pltpu.VMEM((cap, width, width), BF),
                pltpu.VMEM((own, width, width), BF),
                pltpu.VMEM(prev_stats.shape, F32),
                pltpu.VMEM(prev_stats.shape, F32),
                pltpu.VMEM((2 * own, width, width), F32),
                pltpu.VMEM((n_mp - 1, own, part, width), BF),
                pltpu.VMEM((cap, part, width), BF),
                pltpu.VMEM((n_dp, *strip), BF),
                pltpu.VMEM((n_dp, *strip), BF),
                dma, dma, dma, dma((n_mp - 1,)), dma((n_mp - 1,)),
                dma((n_mp - 1,)), dma((n_mp - 1,)),
                dma((n_mp - 1,)), dma((n_mp - 1,)),
                dma((n_mp // 2, own)), dma((n_mp // 2, own)),
                dma((n_mp // 2, own)), dma((n_mp // 2, own)), dma, dma,
            ],
            compiler_params=pltpu.CompilerParams(
                collective_id=0, has_side_effects=True, vmem_limit_bytes=54_100_000
            ),
        )(owner_table, strips, prev_stats)
        update, new_stats, inv_roots = pl.pallas_call(
            write_out,
            out_shape=shapes,
            in_specs=[pl.BlockSpec(memory_space=pl.ANY)] * 3,
            out_specs=(hbm, hbm, hbm),
            scratch_shapes=[dma((3,))],
            compiler_params=pltpu.CompilerParams(vmem_limit_bytes=1 << 20),
        )(*held)
        return jnp.swapaxes(update, 1, 2), new_stats, inv_roots

    return jax.shard_map(
        per_device,
        mesh=mesh,
        in_specs=(P("dp", None, "mp"), P(), P("dp", None, None, None)),
        out_specs=(P("dp", None, "mp"), P("dp", None, None, None), P("dp", None, None, None)),
        check_vma=False,
    )
```

```python
import functools

import jax
import jax.numpy as jnp
from jax import lax
from jax.experimental import pallas as pl
from jax.experimental.pallas import tpu as pltpu
from jax.sharding import PartitionSpec as P

ITERS = 16
STAT_DECAY = 0.75
DAMPING = 0.03
MESH = pl.DeviceIdType.MESH
BF = jnp.bfloat16
F32 = jnp.float32


def eye_of(n, dtype=F32):
    rows = lax.broadcasted_iota(jnp.int32, (n, n), 0)
    cols = lax.broadcasted_iota(jnp.int32, (n, n), 1)
    return (rows == cols).astype(F32).astype(dtype)


def pair(a):
    high = a.astype(BF)
    low = (a - high.astype(F32)).astype(BF)
    return jnp.concatenate([high, low], axis=1)


def twice(a):
    return jnp.concatenate([a, a], axis=0)


def product(left_pair, right_twice):
    out = jnp.dot(left_pair, right_twice, preferred_element_type=F32)
    width = out.shape[1] // 2
    return out[:, :width] + out[:, width:]


def total(a):
    return jnp.sum(jnp.sum(a, axis=1, keepdims=True), axis=0, keepdims=True)


def kernel(
    n_dp, n_mp, owner_ref, grad_ref, prev_hbm,
    upd_ref, nst, inv,
    rank_s, gbuf, hfull, hown, prev, roots, rest, usend, ubuf, obuf, rbuf,
    loc_sem, g_send, g_recv, m_send, m_recv, b_send, b_recv, u_send, u_recv, r_send, r_recv, f_send, f_recv,
    o_send, o_recv,
):
    blk_local, part, width = grad_ref.shape
    cap = prev.shape[0]
    own = cap // n_mp
    nblk = owner_ref.shape[0]
    me = lax.axis_index("dp")
    my = lax.axis_index("mp")
    mate = my + 1 - 2 * lax.rem(my, 2)
    first = own * my
    low_half = me < n_dp // 2

    def rows_of(index):
        return pl.ds(pl.multiple_of(index * part, part), part)

    def slots_of(index):
        return pl.ds(index * own, own)

    def far_first(i):
        return jnp.where(low_half, n_dp - 1 - i, i)

    def offset(d):
        return lax.rem(d - me + n_dp, n_dp)

    def peer(k):
        return lax.rem(my + k, n_mp)

    prev_in = pltpu.make_async_copy(prev_hbm, prev, loc_sem)
    prev_in.start()

    barrier = pltpu.get_barrier_semaphore()

    def greet(k, c):
        pl.semaphore_signal(
            barrier, inc=1, device_id={"dp": lax.rem(me + k, n_dp)}, device_id_type=MESH
        )
        return c

    lax.fori_loop(1, n_dp, greet, 0)
    for k in range(1, n_mp):
        pl.semaphore_signal(barrier, inc=1, device_id={"mp": peer(k)}, device_id_type=MESH)

    my_rows = rows_of(my)
    gbuf[0] = grad_ref[...]

    def scan_table(b, carry):
        count = carry[0]
        mine = owner_ref[b] == me
        rank_s[b] = count
        picked = [
            jnp.where(mine & (count == r), b, carry[1 + r]) for r in range(cap)
        ]
        return (count + mine.astype(jnp.int32), *picked)

    found = lax.fori_loop(0, nblk, scan_table, (jnp.int32(0),) * (cap + 1))
    count, picks = found[0], found[1:]

    pl.semaphore_wait(barrier, n_dp - 1 + n_mp - 1)

    def spread_out(i, c):
        d = far_first(i)

        @pl.when(d != me)
        def _():
            k = offset(d)
            pltpu.make_async_remote_copy(
                src_ref=grad_ref, dst_ref=gbuf.at[k], send_sem=g_send, recv_sem=g_recv,
                device_id={"dp": d}, device_id_type=MESH,
            ).start()

        return c

    lax.fori_loop(0, n_dp, spread_out, 0)
    others = gbuf.at[pl.ds(1, n_dp - 1)]
    pltpu.make_async_copy(others, others, g_recv).wait()

    for r in range(cap):
        home = picks[r] // blk_local
        hfull[r, my_rows, :] = gbuf[
            lax.rem(me - home + n_dp, n_dp), picks[r] - home * blk_local
        ]
    swaps = []
    for sems, whole in (((m_send, m_recv), False), ((b_send, b_recv), True)):
        for k in range(1, n_mp):
            src = hfull.at[:, my_rows, :] if whole else hfull.at[slots_of(peer(k)), my_rows, :]
            swaps.append(pltpu.make_async_remote_copy(
                src_ref=src, dst_ref=src if whole else hown.at[:, my_rows, :],
                send_sem=sems[0].at[k - 1], recv_sem=sems[1].at[k - 1],
                device_id={"mp": peer(k)}, device_id_type=MESH,
            ))
            swaps[-1].start()
    hown[:, my_rows, :] = hfull[slots_of(my), my_rows, :]
    prev_in.wait()

    def collect(buffer, sems):
        for k in range(1, n_mp):
            came = buffer.at[:, rows_of(lax.rem(my - k + n_mp, n_mp)), :]
            pltpu.make_async_copy(came, came, sems.at[k - 1]).wait()

    def blend(h, slot):
        left = lax.dot_general(h, h, (((0,), (0,)), ((), ())), preferred_element_type=F32)
        right = lax.dot_general(h, h, (((1,), (1,)), ((), ())), preferred_element_type=F32)
        return [
            STAT_DECAY * prev[slot, side] + (1.0 - STAT_DECAY) * stat
            for side, stat in ((0, left), (1, right))
        ]

    collect(hown, m_recv)
    eye = eye_of(width)
    slots = [(first + i // 2, i % 2) for i in range(2 * own)]
    span = range(2 * own)
    mixes = [m for i in range(own) for m in blend(hown[i], first + i)]
    for i in span:
        s = jnp.where(slots[i][0] < count, mixes[i], eye)
        a = s + (DAMPING / width) * total(s * eye) * eye
        c = jnp.sqrt(total(a * a))
        roots[slots[i]] = eye * (1.0 / jnp.sqrt(jnp.sqrt(c)))
        rest[i] = a * (1.0 / c)

    def refine(_, carry):
        ident = eye_of(width)
        xs = [roots[slots[i]] for i in span]
        ms = [rest[i] for i in span]
        ml = [pair(m) for m in ms]
        mr = [twice(m) for m in ml]
        out = [product(ml[i], mr[i]) for i in span]
        sq = [
            ident * 1.5625 - ms[i] * 0.625 + out[i] * 0.0625 for i in span
        ]
        sl = [pair(s) for s in sq]
        us = [product(sl[i], mr[i]) for i in span]
        xm = [product(pair(xs[i]), mr[i]) for i in span]
        for i in span:
            roots[slots[i]] = xs[i] * 1.25 - xm[i] * 0.25
        for i in span:
            rest[i] = product(pair(us[i]), twice(sl[i]))
        return carry

    lax.fori_loop(0, ITERS - 1, refine, 0, unroll=3)
    ms = [pair(rest[i]) for i in span]
    out = [product(pair(roots[slots[i]]), twice(ms[i])) for i in span]
    for i in span:
        roots[slots[i]] = roots[slots[i]] * 1.25 - out[i] * 0.25

    def root_copy(src_owner, to, sems, slot):
        part_of = roots.at[src_owner * own + slot]
        return pltpu.make_async_remote_copy(
            src_ref=part_of, dst_ref=part_of, send_sem=sems[0], recv_sem=sems[1],
            device_id={"mp": to}, device_id_type=MESH,
        )

    r0 = [pair(roots[slots[2 * i]]) for i in range(own)]
    r1 = [pair(roots[slots[2 * i + 1]]) for i in range(own)]
    mids = []
    for i in range(own):
        mids.append(jnp.dot(r1[i], twice(hown[i]), preferred_element_type=F32))
    pre = [product(pair(mids[i]), twice(r0[i])) for i in range(own)]
    for i in range(own):
        rms = jnp.sqrt(total(pre[i] * pre[i]) * (1.0 / (width * width)))
        rest[i] = pre[i] * (1.0 / rms)
    for i in range(own):
        for k in range(n_mp):
            rows = rest[i, rows_of(peer(k)), :].astype(BF)
            if k == 0:
                ubuf[first + i] = rows
            else:
                usend[k - 1, i] = rows
    u_swaps = []
    for k in range(1, n_mp):
        u_swaps.append(pltpu.make_async_remote_copy(
            src_ref=usend.at[k - 1], dst_ref=ubuf.at[slots_of(my)],
            send_sem=u_send.at[k - 1], recv_sem=u_recv.at[k - 1],
            device_id={"mp": peer(k)}, device_id_type=MESH,
        ))
        u_swaps[-1].start()
    root_swaps = []
    for i in range(own):
        for j in range(n_mp // 2):
            to = mate if j == 0 else peer(2 * j)
            root_swaps.append(root_copy(my, to, (r_send.at[j, i], r_recv.at[j, i]), i))
            root_swaps[-1].start()
    for k in range(1, n_mp):
        came = ubuf.at[slots_of(lax.rem(my - k + n_mp, n_mp))]
        pltpu.make_async_copy(came, came, u_recv.at[k - 1]).wait()

    def address(k, c):
        home = lax.rem(me + k, n_dp)
        for j in range(blk_local):
            b = home * blk_local + j
            row = jnp.minimum(rank_s[b], cap - 1)
            obuf[k, j] = jnp.where(owner_ref[b] == me, ubuf[row], jnp.zeros((), BF))
        return c

    lax.fori_loop(0, n_dp, address, 0)
    rbuf[0] = obuf[0]

    def give_back(i, c):
        d = far_first(i)

        @pl.when(d != me)
        def _():
            k = offset(d)
            pltpu.make_async_remote_copy(
                src_ref=obuf.at[k], dst_ref=rbuf.at[k], send_sem=o_send, recv_sem=o_recv,
                device_id={"dp": d}, device_id_type=MESH,
            ).start()

        return c

    lax.fori_loop(0, n_dp, give_back, 0)

    collect(hfull, b_recv)
    for r in range(cap):
        for side, mix in enumerate(blend(hfull[r], r)):
            nst[r, side] = jnp.where(r < count, mix, 0.0)

    def keep(slot):
        for side in range(2):
            inv[slot, side] = jnp.where(slot < count, roots[slot, side], 0.0)

    def arrive(source, i, sem):
        came = roots.at[source * own + i]
        pltpu.make_async_copy(came, came, sem).wait()

    for i in range(own):
        keep(first + i)
        arrive(mate, i, r_recv.at[0, i])
        keep(mate * own + i)
    for i in range(own):
        for j in range(1, n_mp // 2):
            source = lax.rem(my - 2 * j + n_mp, n_mp)
            arrive(source, i, r_recv.at[j, i])
            root_swaps.append(root_copy(source, mate, (f_send.at[j - 1, i], f_recv.at[j - 1, i]), i))
            root_swaps[-1].start()
            keep(source * own + i)
    for i in range(own):
        for j in range(1, n_mp // 2):
            source = lax.rem(mate - 2 * j + n_mp, n_mp)
            arrive(source, i, f_recv.at[j - 1, i])
            keep(source * own + i)

    back = rbuf.at[pl.ds(1, n_dp - 1)]
    pltpu.make_async_copy(back, back, o_recv).wait()
    for j in range(blk_local):
        owner = owner_ref[me * blk_local + j]
        got = rbuf[lax.rem(me - owner + n_dp, n_dp), j]
        upd_ref[j] = got

    for swap in swaps + u_swaps + root_swaps:
        swap.wait_send()
    pltpu.make_async_copy(others, others, g_send).wait()
    pltpu.make_async_copy(back, back, o_send).wait()


def write_out(upd, nst, inv, upd_out, nst_out, inv_out, sems):
    copies = [
        pltpu.make_async_copy(src, dst, sems.at[i])
        for i, (src, dst) in enumerate(((nst, nst_out), (inv, inv_out), (upd, upd_out)))
    ]
    for copy in copies:
        copy.start()
    for copy in copies:
        copy.wait()


def solution(mesh):
    n_dp, n_mp = mesh.shape["dp"], mesh.shape["mp"]

    def per_device(grad_blocks, owner_table, prev_stats):
        strips = jnp.swapaxes(grad_blocks, 1, 2)
        blk_local, part, width = strips.shape
        cap = prev_stats.shape[0]
        own = cap // n_mp
        vmem = pl.BlockSpec(memory_space=pltpu.VMEM)
        hbm = pl.BlockSpec(memory_space=pltpu.HBM)
        strip = strips.shape
        dma = pltpu.SemaphoreType.DMA
        shapes = (
            jax.ShapeDtypeStruct(strip, BF),
            jax.ShapeDtypeStruct(prev_stats.shape, F32),
            jax.ShapeDtypeStruct(prev_stats.shape, F32),
        )
        held = pl.pallas_call(
            functools.partial(kernel, n_dp, n_mp),
            out_shape=shapes,
            in_specs=[pl.BlockSpec(memory_space=pltpu.SMEM), vmem, hbm],
            out_specs=(vmem, vmem, vmem),
            scratch_shapes=[
                pltpu.SMEM((owner_table.shape[0],), jnp.int32),
                pltpu.VMEM((n_dp, *strip), BF),
                pltpu.VMEM((cap, width, width), BF),
                pltpu.VMEM((own, width, width), BF),
                pltpu.VMEM(prev_stats.shape, F32),
                pltpu.VMEM(prev_stats.shape, F32),
                pltpu.VMEM((2 * own, width, width), F32),
                pltpu.VMEM((n_mp - 1, own, part, width), BF),
                pltpu.VMEM((cap, part, width), BF),
                pltpu.VMEM((n_dp, *strip), BF),
                pltpu.VMEM((n_dp, *strip), BF),
                dma, dma, dma, dma((n_mp - 1,)), dma((n_mp - 1,)),
                dma((n_mp - 1,)), dma((n_mp - 1,)),
                dma((n_mp - 1,)), dma((n_mp - 1,)),
                dma((n_mp // 2, own)), dma((n_mp // 2, own)),
                dma((n_mp // 2, own)), dma((n_mp // 2, own)), dma, dma,
            ],
            compiler_params=pltpu.CompilerParams(
                collective_id=0, has_side_effects=True, vmem_limit_bytes=54_100_000
            ),
        )(owner_table, strips, prev_stats)
        update, new_stats, inv_roots = pl.pallas_call(
            write_out,
            out_shape=shapes,
            in_specs=[pl.BlockSpec(memory_space=pl.ANY)] * 3,
            out_specs=(hbm, hbm, hbm),
            scratch_shapes=[dma((3,))],
            compiler_params=pltpu.CompilerParams(vmem_limit_bytes=1 << 20),
        )(*held)
        return jnp.swapaxes(update, 1, 2), new_stats, inv_roots

    return jax.shard_map(
        per_device,
        mesh=mesh,
        in_specs=(P("dp", None, "mp"), P(), P("dp", None, None, None)),
        out_specs=(P("dp", None, "mp"), P("dp", None, None, None), P("dp", None, None, None)),
        check_vma=False,
    )
```

```python
import functools

import jax
import jax.numpy as jnp
from jax import lax
from jax.experimental import pallas as pl
from jax.experimental.pallas import tpu as pltpu
from jax.sharding import PartitionSpec as P

ITERS = 16
STAT_DECAY = 0.75
DAMPING = 0.03
MESH = pl.DeviceIdType.MESH
BF = jnp.bfloat16
F32 = jnp.float32


def eye_of(n, dtype=F32):
    rows = lax.broadcasted_iota(jnp.int32, (n, n), 0)
    cols = lax.broadcasted_iota(jnp.int32, (n, n), 1)
    return (rows == cols).astype(F32).astype(dtype)


def pair(a):
    high = a.astype(BF)
    low = (a - high.astype(F32)).astype(BF)
    return jnp.concatenate([high, low], axis=1)


def twice(a):
    return jnp.concatenate([a, a], axis=0)


def product(left_pair, right_twice):
    out = jnp.dot(left_pair, right_twice, preferred_element_type=F32)
    width = out.shape[1] // 2
    return out[:, :width] + out[:, width:]


def total(a):
    return jnp.sum(jnp.sum(a, axis=1, keepdims=True), axis=0, keepdims=True)


def kernel(
    n_dp, n_mp, owner_ref, grad_ref, prev_hbm,
    upd_ref, nst, inv,
    rank_s, gbuf, hfull, hown, prev, roots, rest, usend, ubuf, obuf, rbuf,
    loc_sem, g_send, g_recv, m_send, m_recv, b_send, b_recv, u_send, u_recv, r_send, r_recv, f_send, f_recv,
    o_send, o_recv,
):
    blk_local, part, width = grad_ref.shape
    cap = prev.shape[0]
    own = cap // n_mp
    nblk = owner_ref.shape[0]
    me = lax.axis_index("dp")
    my = lax.axis_index("mp")
    mate = my + 1 - 2 * lax.rem(my, 2)
    first = own * my
    low_half = me < n_dp // 2

    def rows_of(index):
        return pl.ds(pl.multiple_of(index * part, part), part)

    def slots_of(index):
        return pl.ds(index * own, own)

    def far_first(i):
        return jnp.where(low_half, n_dp - 1 - i, i)

    def offset(d):
        return lax.rem(d - me + n_dp, n_dp)

    def peer(k):
        return lax.rem(my + k, n_mp)

    prev_in = pltpu.make_async_copy(prev_hbm, prev, loc_sem)
    prev_in.start()

    barrier = pltpu.get_barrier_semaphore()

    def greet(k, c):
        pl.semaphore_signal(
            barrier, inc=1, device_id={"dp": lax.rem(me + k, n_dp)}, device_id_type=MESH
        )
        return c

    lax.fori_loop(1, n_dp, greet, 0)
    for k in range(1, n_mp):
        pl.semaphore_signal(barrier, inc=1, device_id={"mp": peer(k)}, device_id_type=MESH)

    my_rows = rows_of(my)
    gbuf[0] = grad_ref[...]

    def scan_table(b, carry):
        count = carry[0]
        mine = owner_ref[b] == me
        rank_s[b] = count
        picked = [
            jnp.where(mine & (count == r), b, carry[1 + r]) for r in range(cap)
        ]
        return (count + mine.astype(jnp.int32), *picked)

    found = lax.fori_loop(0, nblk, scan_table, (jnp.int32(0),) * (cap + 1))
    count, picks = found[0], found[1:]

    pl.semaphore_wait(barrier, n_dp - 1 + n_mp - 1)

    def spread_out(i, c):
        d = far_first(i)

        @pl.when(d != me)
        def _():
            k = offset(d)
            pltpu.make_async_remote_copy(
                src_ref=grad_ref, dst_ref=gbuf.at[k], send_sem=g_send, recv_sem=g_recv,
                device_id={"dp": d}, device_id_type=MESH,
            ).start()

        return c

    lax.fori_loop(0, n_dp, spread_out, 0)
    others = gbuf.at[pl.ds(1, n_dp - 1)]
    pltpu.make_async_copy(others, others, g_recv).wait()

    for r in range(cap):
        home = picks[r] // blk_local
        hfull[r, my_rows, :] = gbuf[
            lax.rem(me - home + n_dp, n_dp), picks[r] - home * blk_local
        ]
    swaps = []
    for sems, whole in (((m_send, m_recv), False), ((b_send, b_recv), True)):
        for k in range(1, n_mp):
            src = hfull.at[:, my_rows, :] if whole else hfull.at[slots_of(peer(k)), my_rows, :]
            swaps.append(pltpu.make_async_remote_copy(
                src_ref=src, dst_ref=src if whole else hown.at[:, my_rows, :],
                send_sem=sems[0].at[k - 1], recv_sem=sems[1].at[k - 1],
                device_id={"mp": peer(k)}, device_id_type=MESH,
            ))
            swaps[-1].start()
    hown[:, my_rows, :] = hfull[slots_of(my), my_rows, :]
    prev_in.wait()

    def collect(buffer, sems):
        for k in range(1, n_mp):
            came = buffer.at[:, rows_of(lax.rem(my - k + n_mp, n_mp)), :]
            pltpu.make_async_copy(came, came, sems.at[k - 1]).wait()

    def blend(h, slot):
        left = lax.dot_general(h, h, (((0,), (0,)), ((), ())), preferred_element_type=F32)
        right = lax.dot_general(h, h, (((1,), (1,)), ((), ())), preferred_element_type=F32)
        return [
            STAT_DECAY * prev[slot, side] + (1.0 - STAT_DECAY) * stat
            for side, stat in ((0, left), (1, right))
        ]

    collect(hown, m_recv)
    eye = eye_of(width)
    slots = [(first + i // 2, i % 2) for i in range(2 * own)]
    span = range(2 * own)
    mixes = [m for i in range(own) for m in blend(hown[i], first + i)]
    for i in span:
        s = jnp.where(slots[i][0] < count, mixes[i], eye)
        a = s + (DAMPING / width) * total(s * eye) * eye
        c = jnp.sqrt(total(a * a))
        roots[slots[i]] = eye * (1.0 / jnp.sqrt(jnp.sqrt(c)))
        rest[i] = a * (1.0 / c)

    def refine(_, carry):
        ident = eye_of(width)
        xs = [roots[slots[i]] for i in span]
        ms = [rest[i] for i in span]
        ml = [pair(m) for m in ms]
        mr = [twice(m) for m in ml]
        out = [product(ml[i], mr[i]) for i in span]
        sq = [
            ident * 1.5625 - ms[i] * 0.625 + out[i] * 0.0625 for i in span
        ]
        sl = [pair(s) for s in sq]
        us = [product(sl[i], mr[i]) for i in span]
        xm = [product(pair(xs[i]), mr[i]) for i in span]
        for i in span:
            roots[slots[i]] = xs[i] * 1.25 - xm[i] * 0.25
        for i in span:
            rest[i] = product(pair(us[i]), twice(sl[i]))
        return carry

    lax.fori_loop(0, ITERS - 1, refine, 0, unroll=5)
    ms = [pair(rest[i]) for i in span]
    out = [product(pair(roots[slots[i]]), twice(ms[i])) for i in span]
    for i in span:
        roots[slots[i]] = roots[slots[i]] * 1.25 - out[i] * 0.25

    def root_copy(src_owner, to, sems, slot):
        part_of = roots.at[src_owner * own + slot]
        return pltpu.make_async_remote_copy(
            src_ref=part_of, dst_ref=part_of, send_sem=sems[0], recv_sem=sems[1],
            device_id={"mp": to}, device_id_type=MESH,
        )

    r0 = [pair(roots[slots[2 * i]]) for i in range(own)]
    r1 = [pair(roots[slots[2 * i + 1]]) for i in range(own)]
    mids = []
    for i in range(own):
        mids.append(jnp.dot(r1[i], twice(hown[i]), preferred_element_type=F32))
    pre = [product(pair(mids[i]), twice(r0[i])) for i in range(own)]
    for i in range(own):
        rms = jnp.sqrt(total(pre[i] * pre[i]) * (1.0 / (width * width)))
        rest[i] = pre[i] / rms
    for i in range(own):
        for k in range(n_mp):
            rows = rest[i, rows_of(peer(k)), :].astype(BF)
            if k == 0:
                ubuf[first + i] = rows
            else:
                usend[k - 1, i] = rows
    u_swaps = []
    for k in range(1, n_mp):
        u_swaps.append(pltpu.make_async_remote_copy(
            src_ref=usend.at[k - 1], dst_ref=ubuf.at[slots_of(my)],
            send_sem=u_send.at[k - 1], recv_sem=u_recv.at[k - 1],
            device_id={"mp": peer(k)}, device_id_type=MESH,
        ))
        u_swaps[-1].start()
    root_swaps = []
    for i in range(own):
        for j in reversed(range(n_mp // 2)):
            to = mate if j == 0 else peer(2 * j)
            root_swaps.append(root_copy(my, to, (r_send.at[j, i], r_recv.at[j, i]), i))
            root_swaps[-1].start()
    for k in range(1, n_mp):
        came = ubuf.at[slots_of(lax.rem(my - k + n_mp, n_mp))]
        pltpu.make_async_copy(came, came, u_recv.at[k - 1]).wait()

    def address(k, c):
        home = lax.rem(me + k, n_dp)
        for j in range(blk_local):
            b = home * blk_local + j
            row = jnp.minimum(rank_s[b], cap - 1)
            obuf[k, j] = jnp.where(owner_ref[b] == me, ubuf[row], jnp.zeros((), BF))
        return c

    lax.fori_loop(0, n_dp, address, 0)
    rbuf[0] = obuf[0]

    def give_back(i, c):
        d = far_first(i)

        @pl.when(d != me)
        def _():
            k = offset(d)
            pltpu.make_async_remote_copy(
                src_ref=obuf.at[k], dst_ref=rbuf.at[k], send_sem=o_send, recv_sem=o_recv,
                device_id={"dp": d}, device_id_type=MESH,
            ).start()

        return c

    lax.fori_loop(0, n_dp, give_back, 0)

    collect(hfull, b_recv)
    for r in range(cap):
        for side, mix in enumerate(blend(hfull[r], r)):
            nst[r, side] = jnp.where(r < count, mix, 0.0)

    for i in range(own):
        for j in range(1, n_mp // 2):
            source = lax.rem(my - 2 * j + n_mp, n_mp)
            came = roots.at[source * own + i]
            pltpu.make_async_copy(came, came, r_recv.at[j, i]).wait()
            root_swaps.append(root_copy(source, mate, (f_send.at[j - 1, i], f_recv.at[j - 1, i]), i))
            root_swaps[-1].start()
    for i in range(own):
        for j in range(n_mp // 2):
            source = lax.rem(mate - 2 * j + n_mp, n_mp)
            came = roots.at[source * own + i]
            sem = r_recv.at[0, i] if j == 0 else f_recv.at[j - 1, i]
            pltpu.make_async_copy(came, came, sem).wait()
    for r in range(cap):
        for side in range(2):
            inv[r, side] = jnp.where(r < count, roots[r, side], 0.0)

    back = rbuf.at[pl.ds(1, n_dp - 1)]
    pltpu.make_async_copy(back, back, o_recv).wait()
    for j in range(blk_local):
        owner = owner_ref[me * blk_local + j]
        got = rbuf[lax.rem(me - owner + n_dp, n_dp), j]
        upd_ref[j] = got

    for swap in swaps + u_swaps + root_swaps:
        swap.wait_send()
    pltpu.make_async_copy(others, others, g_send).wait()
    pltpu.make_async_copy(back, back, o_send).wait()


def write_out(upd, nst, inv, upd_out, nst_out, inv_out, sems):
    copies = [
        pltpu.make_async_copy(src, dst, sems.at[i])
        for i, (src, dst) in enumerate(((nst, nst_out), (inv, inv_out), (upd, upd_out)))
    ]
    for copy in copies:
        copy.start()
    for copy in copies:
        copy.wait()


def solution(mesh):
    n_dp, n_mp = mesh.shape["dp"], mesh.shape["mp"]

    def per_device(grad_blocks, owner_table, prev_stats):
        strips = jnp.swapaxes(grad_blocks, 1, 2)
        blk_local, part, width = strips.shape
        cap = prev_stats.shape[0]
        own = cap // n_mp
        vmem = pl.BlockSpec(memory_space=pltpu.VMEM)
        hbm = pl.BlockSpec(memory_space=pltpu.HBM)
        strip = strips.shape
        dma = pltpu.SemaphoreType.DMA
        shapes = (
            jax.ShapeDtypeStruct(strip, BF),
            jax.ShapeDtypeStruct(prev_stats.shape, F32),
            jax.ShapeDtypeStruct(prev_stats.shape, F32),
        )
        held = pl.pallas_call(
            functools.partial(kernel, n_dp, n_mp),
            out_shape=shapes,
            in_specs=[pl.BlockSpec(memory_space=pltpu.SMEM), vmem, hbm],
            out_specs=(vmem, vmem, vmem),
            scratch_shapes=[
                pltpu.SMEM((owner_table.shape[0],), jnp.int32),
                pltpu.VMEM((n_dp, *strip), BF),
                pltpu.VMEM((cap, width, width), BF),
                pltpu.VMEM((own, width, width), BF),
                pltpu.VMEM(prev_stats.shape, F32),
                pltpu.VMEM(prev_stats.shape, F32),
                pltpu.VMEM((2 * own, width, width), F32),
                pltpu.VMEM((n_mp - 1, own, part, width), BF),
                pltpu.VMEM((cap, part, width), BF),
                pltpu.VMEM((n_dp, *strip), BF),
                pltpu.VMEM((n_dp, *strip), BF),
                dma, dma, dma, dma((n_mp - 1,)), dma((n_mp - 1,)),
                dma((n_mp - 1,)), dma((n_mp - 1,)),
                dma((n_mp - 1,)), dma((n_mp - 1,)),
                dma((n_mp // 2, own)), dma((n_mp // 2, own)),
                dma((n_mp // 2, own)), dma((n_mp // 2, own)), dma, dma,
            ],
            compiler_params=pltpu.CompilerParams(
                collective_id=0, has_side_effects=True, vmem_limit_bytes=54_100_000
            ),
        )(owner_table, strips, prev_stats)
        update, new_stats, inv_roots = pl.pallas_call(
            write_out,
            out_shape=shapes,
            in_specs=[pl.BlockSpec(memory_space=pl.ANY)] * 3,
            out_specs=(hbm, hbm, hbm),
            scratch_shapes=[dma((3,))],
            compiler_params=pltpu.CompilerParams(vmem_limit_bytes=1 << 20),
        )(*held)
        return jnp.swapaxes(update, 1, 2), new_stats, inv_roots

    return jax.shard_map(
        per_device,
        mesh=mesh,
        in_specs=(P("dp", None, "mp"), P(), P("dp", None, None, None)),
        out_specs=(P("dp", None, "mp"), P("dp", None, None, None), P("dp", None, None, None)),
        check_vma=False,
    )
```
